32 devices in a mesh: group: 2 (over y), expert: 4 (over x, core), tensor: 4 (over z).
Axes of the slice: x: 2, y: 2, z: 4, core: 2. Of those that a mesh axis runs over, the one named last changes fastest.
Arguments:
- tokens: bfloat16 [512, 4096], P(('group', 'expert'), 'tensor'), parts along dimension 0, may hold values from -6 to 6
- w_gate: bfloat16 [8, 4096, 1536], P('expert', 'tensor'), may hold values from -0.125 to 0.125
- w_up: bfloat16 [8, 4096, 1536], P('expert', 'tensor'), may hold values from -0.125 to 0.125
- w_down: bfloat16 [8, 1536, 4096], P('expert', None, 'tensor'), may hold values from -0.15625 to 0.15625
- expert_ids: int32 [512, 8], P(('group', 'expert')), parts along dimension 0, may hold values from 0 to 7, as said below
- route_weights: float32 [512, 8], P(('group', 'expert')), parts along dimension 0, may hold values from 0.05 to 0.5
Outputs:
- mixed_out: bfloat16 [512, 4096], P(('group', 'expert'), 'tensor'), parts along dimension 0
The draws below stay inside these ranges and needn't reach their ends.
There are 2 independent parts, one for each index of `group`. The reference program is written for one: setup_inputs(seed, part) draws one part's arguments, and reference() takes and returns one part's arrays. A program takes and returns all parts, laid end to end along the dimension named above; an argument that names none is the same for every part. Nothing has to cross between parts.
Inputs may be any that keep to these rules, and one draw needn't show every extreme that they name: `expert_ids`: each row names 8 different experts. In each aligned block of 64 rows no expert is named by more than 64 rows, and one expert, the same in every block of a part, is named by exactly 64 rows of every block.
All inputs are finite; a program needn't handle non-finite values.
Results may differ from the reference program's by a relative error of at most 0.0057.
Values may be sent and summed in bfloat16 or wider, within the bound.
A program may use at most 128 MiB of HBM per device.

```python
import math
import jax
import jax.numpy as jnp
from jax import lax

D = 4096
FF = 1536
TOP = 8
TOK_DEV = 64
EXPERTS = 8
TOKENS = 256
BLOCKS = 4
CAP = 64


def expert_of(ordinal, hot_expert):
    return ordinal + (ordinal >= hot_expert).astype(jnp.int32)


def draw_expert_ids(key, part):
    hot_expert = jax.random.randint(jax.random.fold_in(key, 11), (), 0, EXPERTS, dtype=jnp.int32)
    pool_size = (EXPERTS - 1) * CAP
    deficit_total = EXPERTS * CAP - TOK_DEV * TOP
    block_keys = jax.random.split(jax.random.fold_in(key, 12), BLOCKS)

    def column_order(column_key):
        return jax.random.permutation(column_key, TOP).astype(jnp.int32)

    def one_block(block_key):
        sub_keys = jax.random.split(block_key, 3)
        shuffled = jax.random.permutation(sub_keys[0], pool_size).astype(jnp.int32)
        chosen = shuffled[:deficit_total] // CAP
        labels = jnp.arange(EXPERTS - 1, dtype=jnp.int32)
        deficit = jnp.sum((chosen[:, None] == labels[None, :]).astype(jnp.int32), axis=0)
        others = CAP - deficit
        counts = jnp.zeros((EXPERTS,), jnp.int32).at[expert_of(labels, hot_expert)].set(others)
        counts = counts.at[hot_expert].set(CAP)
        run_ends = jnp.cumsum(counts)
        position = jnp.arange(TOK_DEV * TOP, dtype=jnp.int32)
        sequence = jnp.sum((run_ends[None, :] <= position[:, None]).astype(jnp.int32), axis=1)
        layout = sequence.reshape(TOP, TOK_DEV).T
        row_order = jax.random.permutation(sub_keys[1], TOK_DEV).astype(jnp.int32)
        layout = layout[row_order]
        columns = jax.vmap(column_order)(jax.random.split(sub_keys[2], TOK_DEV))
        return jnp.take_along_axis(layout, columns, axis=1)
    return jax.vmap(one_block)(block_keys).reshape(TOKENS, TOP).astype(jnp.int32)


def with_spikes(entries, stream_key, source, target, shards_of, factor):
    owner, partner = [(jnp.arange(entries.shape[dim]) // (entries.shape[dim] // shards_of)).reshape([-1 if axis == dim else 1 for axis in range(entries.ndim)]) for dim in (source, target)]
    chosen = jax.random.permutation(stream_key, shards_of)[partner]
    strong = (owner == chosen) | (owner == (partner + shards_of // 2) % shards_of)
    return jnp.where(strong, factor * entries, entries)


def levels(own_key, shape, cuts, least, top_value):
    loudness, own = 1.0, jax.random.fold_in(own_key, 6)
    for dim, blocks in cuts:
        heights = jnp.exp(jax.random.uniform(jax.random.fold_in(own, dim), (blocks,), jnp.float32, least / len(cuts), top_value / len(cuts)))
        loudness = loudness * jnp.repeat(heights, shape[dim] // blocks).reshape([-1 if axis == dim else 1 for axis in range(len(shape))])
    return loudness


def scatter_about(rng, dims, width, bound, cuts=(), held_as=jnp.bfloat16):
    result = jax.random.normal(rng, dims, jnp.float32) * width
    if len(cuts) > 0:
        result = levels(rng, dims, cuts, -0.22, 0.18) * result
    return jnp.clip(result, min=-bound, max=bound).astype(held_as)


def bell_draw_with(rng, extent, deviation, bound, pieces, heavy, kind=jnp.bfloat16):
    values = deviation * jax.random.normal(rng, extent, jnp.float32)
    if pieces:
        values = values * levels(rng, extent, pieces, -0.22, 0.18)
    return jnp.clip(with_spikes(values, jax.random.fold_in(rng, 3), *heavy), -bound, bound).astype(kind)


def setup_inputs(seed: int = 0, part: int = 0) -> dict:
    keys = jax.random.split(jax.random.key(seed), 7)
    part_splits = jax.random.split(jax.random.fold_in(keys[6], part), 7)
    tokens = scatter_about(part_splits[0], (TOKENS, D), 1.0, 6.0, ((0, 4), (1, 4)))
    w_gate = bell_draw_with(keys[1], (EXPERTS, D, FF), D ** -0.5, 0.125, ((0, 4), (1, 4)), (1, 2, 4, 2.0))
    w_up = bell_draw_with(keys[2], (EXPERTS, D, FF), D ** -0.5, 0.125, ((0, 4), (1, 4)), (1, 2, 4, 2.0))
    w_down = scatter_about(keys[3], (EXPERTS, FF, D), FF ** -0.5, 0.15625, ((0, 4), (2, 4)))
    expert_ids = draw_expert_ids(jax.random.fold_in(jax.random.fold_in(keys[6], part), 71), part)
    route_weights = jnp.clip(jnp.exp(math.log(0.5) - 2.3025851 * jax.random.uniform(part_splits[5], (TOKENS, TOP), jnp.float32) ** levels(part_splits[5], (TOKENS, TOP), ((0, 4),), -0.2, 0.2)), 0.05, 0.5)
    return dict(tokens=tokens, w_gate=w_gate, w_up=w_up, w_down=w_down, expert_ids=expert_ids, route_weights=route_weights)


def slot_numbers(expert_ids):
    flat_ids = expert_ids.reshape(BLOCKS, TOK_DEV * TOP)
    labels = jnp.arange(EXPERTS, dtype=jnp.int32)
    onehot = (flat_ids[:, :, None] == labels[None, None, :]).astype(jnp.int32)
    before = jnp.cumsum(onehot, axis=1) - onehot
    return jnp.sum(before * onehot, axis=2).reshape(TOKENS, TOP).astype(jnp.int32)


def expert_block(operands):
    row_block, gate_w, up_w, down_w = operands
    gate = jnp.dot(row_block, gate_w, preferred_element_type=jnp.float32)
    up = jnp.dot(row_block, up_w, preferred_element_type=jnp.float32)
    hidden = (jax.nn.silu(gate) * up).astype(jnp.bfloat16)
    return jnp.dot(hidden, down_w, preferred_element_type=jnp.float32).astype(jnp.bfloat16)


def reference(tokens, w_gate, w_up, w_down, expert_ids, route_weights):
    slot_ids = slot_numbers(expert_ids)
    block_ids = (jnp.arange(TOKENS, dtype=jnp.int32) // TOK_DEV)[:, None] * jnp.ones((1, TOP), jnp.int32)
    position = ((expert_ids * BLOCKS + block_ids) * CAP + slot_ids).reshape(TOKENS * TOP).astype(jnp.int32)
    owners = (jnp.arange(TOKENS, dtype=jnp.int32)[:, None] * jnp.ones((1, TOP), jnp.int32)).reshape(TOKENS * TOP)
    source = jnp.full((EXPERTS * BLOCKS * CAP,), -1, jnp.int32).at[position].set(owners)
    gathered = tokens[jnp.maximum(source, 0)]
    expert_input = jnp.where((source >= 0)[:, None], gathered, jnp.zeros((), jnp.bfloat16))
    expert_input = expert_input.reshape(EXPERTS, BLOCKS * CAP, D)
    expert_output = lax.map(expert_block, (expert_input, w_gate, w_up, w_down))
    expert_output = expert_output.reshape(EXPERTS * BLOCKS * CAP, D)
    picked = expert_output[position].reshape(TOKENS, TOP, D).astype(jnp.float32)
    mixed_out = jnp.sum(picked * route_weights[:, :, None], axis=1)
    return mixed_out.astype(jnp.bfloat16)
```

```python
import functools

import jax
import jax.numpy as jnp
from jax import lax
from jax.experimental import pallas as pl
from jax.experimental.pallas import tpu as pltpu
from jax.sharding import PartitionSpec as P


def slot_numbers(flat_ids, experts_all):
    labels = jnp.arange(experts_all, dtype=jnp.int32)
    onehot = (flat_ids[:, None] == labels[None, :]).astype(jnp.int32)
    before = jnp.cumsum(onehot, axis=0) - onehot
    return jnp.sum(before * onehot, axis=1)


def routed_by_slots(tokens, w_gate, w_up, w_down, expert_ids, route_weights):
    n_expert = lax.axis_size("expert")
    held_experts = w_gate.shape[0]
    experts_all = held_experts * n_expert
    tok_rows = tokens.shape[0]
    col_share = tokens.shape[1]
    per_token = expert_ids.shape[1]
    capacity = min(tok_rows, 2 * tok_rows * per_token // experts_all)
    flat_ids = expert_ids.reshape(tok_rows * per_token)
    position = flat_ids * capacity + slot_numbers(flat_ids, experts_all)
    owners = jnp.arange(tok_rows * per_token, dtype=jnp.int32) // per_token
    source = jnp.full((experts_all * capacity,), -1, jnp.int32).at[position].set(owners)
    filled = (source >= 0)[:, None]
    picked_rows = jnp.where(filled, tokens[jnp.maximum(source, 0)], jnp.zeros((), tokens.dtype))
    outgoing = picked_rows.reshape(n_expert, held_experts, capacity, col_share)
    received = lax.all_to_all(outgoing, "expert", split_axis=0, concat_axis=0, tiled=True)
    gate_part = jnp.einsum("sjnd,jdf->sjnf", received, w_gate, preferred_element_type=jnp.float32)
    up_part = jnp.einsum("sjnd,jdf->sjnf", received, w_up, preferred_element_type=jnp.float32)
    gate_share = lax.psum_scatter(gate_part, "tensor", scatter_dimension=3, tiled=True)
    up_share = lax.psum_scatter(up_part, "tensor", scatter_dimension=3, tiled=True)
    hidden_share = (jax.nn.silu(gate_share) * up_share).astype(jnp.bfloat16)
    hidden = lax.all_gather(hidden_share, "tensor", axis=3, tiled=True)
    result = jnp.einsum("sjnf,jfd->sjnd", hidden, w_down, preferred_element_type=jnp.float32)
    returned = result.astype(jnp.bfloat16)
    combined = lax.all_to_all(returned, "expert", split_axis=0, concat_axis=0, tiled=True).reshape(
        experts_all * capacity, col_share
    )
    picked = combined[position].reshape(tok_rows, per_token, col_share).astype(jnp.float32)
    mixed_out = jnp.sum(picked * route_weights[:, :, None], axis=1)
    return mixed_out.astype(jnp.bfloat16)


LANES = 128
RS_LAG = 2
AG_LAG = 2
OUT_CHUNKS = 4
MESH = pl.DeviceIdType.MESH


def layer_kernel(
    n_expert, n_tensor, tok_ref, route_ref, wg_hbm, wu_hbm, wd_hbm, out_ref,
    rows_ref, routes_ref, scale_ref, wg_ref, wu_ref, wd_ref, part_ref, sent_ref, got_ref, hidden_ref,
    own_ref, ret_out_ref, ret_in_ref,
    w_sem, tok_send, tok_recv, route_send, route_recv, rs_send, rs_recv, ag_send, ag_recv, ret_send, ret_recv,
):
    held, depth, ff = wg_ref.shape
    tok_rows, cols = tok_ref.shape
    all_rows = n_expert * tok_rows
    per_expert = ff // LANES
    items = held * per_expert // 2
    me = lax.axis_index("expert")
    at = lax.axis_index("tensor")
    last = n_tensor - 1
    peers = [lax.rem(me + k, n_expert) for k in range(1, n_expert)]

    loads = []
    for j in range(held):
        for k, (hbm, vmem) in enumerate(((wg_hbm, wg_ref), (wu_hbm, wu_ref))):
            loads.append(pltpu.make_async_copy(hbm.at[j], vmem.at[j], w_sem.at[2 * j + k]))
    loads.append(pltpu.make_async_copy(wd_hbm, wd_ref, w_sem.at[2 * held]))
    for load in loads:
        load.start()

    barrier = pltpu.get_barrier_semaphore()
    for peer in peers:
        pl.semaphore_signal(barrier, inc=1, device_id={"expert": peer}, device_id_type=MESH)

    @pl.when(at > 0)
    def _():
        pl.semaphore_signal(barrier, inc=1, device_id={"tensor": at - 1}, device_id_type=MESH)

    @pl.when(at < last)
    def _():
        pl.semaphore_signal(barrier, inc=1, device_id={"tensor": at + 1}, device_id_type=MESH)

    greeted = (n_expert - 1) + (at > 0).astype(jnp.int32) + (at < last).astype(jnp.int32)
    pl.semaphore_wait(barrier, greeted)

    def tok_copy(k, slot):
        return pltpu.make_async_remote_copy(
            src_ref=tok_ref, dst_ref=rows_ref.at[slot], send_sem=tok_send.at[k], recv_sem=tok_recv.at[slot],
            device_id={"expert": peers[k]}, device_id_type=MESH)

    def route_copy(k, slot):
        return pltpu.make_async_remote_copy(
            src_ref=route_ref, dst_ref=routes_ref.at[slot], send_sem=route_send.at[k], recv_sem=route_recv.at[slot],
            device_id={"expert": peers[k]}, device_id_type=MESH)

    for k in range(n_expert - 1):
        tok_copy(k, me).start()
    for k in range(n_expert - 1):
        route_copy(k, me).start()
    rows_ref[me] = tok_ref[...]
    routes_ref[me] = route_ref[...]
    for load in loads[:-1]:
        load.wait()
    for k in range(n_expert - 1):
        tok_copy(k, peers[k]).wait_recv()
    for k in range(n_expert - 1):
        route_copy(k, peers[k]).wait_recv()
    routes = routes_ref[...].reshape(all_rows, LANES)
    lane = lax.broadcasted_iota(jnp.int32, (all_rows, LANES), 1)
    for j in range(held):
        mine = jnp.sum(jnp.where(lane == me * held + j, routes, 0.0), axis=1, keepdims=True)
        scale_ref[j] = jnp.broadcast_to(mine, (all_rows, LANES))

    far = (last - at, at)
    onward = (jnp.maximum(at - 1, 0), jnp.minimum(at + 1, last))
    back = (jnp.minimum(at + 1, last), jnp.maximum(at - 1, 0))

    def rs_copy(f, i):
        return pltpu.make_async_remote_copy(
            src_ref=sent_ref.at[f, i], dst_ref=got_ref.at[f, i], send_sem=rs_send.at[f, i], recv_sem=rs_recv.at[f, i],
            device_id={"tensor": onward[f]}, device_id_type=MESH)

    def ag_copy(f, i):
        return pltpu.make_async_remote_copy(
            src_ref=hidden_ref.at[f, i], dst_ref=hidden_ref.at[f, i], send_sem=ag_send.at[f, i],
            recv_sem=ag_recv.at[f, i], device_id={"tensor": back[f]}, device_id_type=MESH)

    def compute_part(f, i):
        q = f * items + i
        j = q // per_expert
        start = pl.multiple_of(lax.rem(q, per_expert) * LANES, LANES)
        both = jnp.concatenate([wg_ref[j, :, pl.ds(start, LANES)], wu_ref[j, :, pl.ds(start, LANES)]], axis=1)
        part_ref[f] = jnp.dot(rows_ref[...].reshape(all_rows, depth), both, preferred_element_type=jnp.float32)

    def finish_part(f, i):
        @pl.when(far[f] > 0)
        def _():
            rs_copy(f, i).wait_recv()
            part_ref[f] = part_ref[f] + got_ref[f, i].astype(jnp.float32)

        @pl.when(far[f] < last)
        def _():
            sent_ref[f, i] = part_ref[f].astype(jnp.bfloat16)
            rs_copy(f, i).start()

        @pl.when(far[f] == last)
        def _():
            gate = part_ref[f, :, :LANES]
            up = part_ref[f, :, LANES:]
            j = (f * items + i) // per_expert
            hidden_ref[f, i] = (jax.nn.silu(gate) * up * scale_ref[j]).astype(jnp.bfloat16)
            ag_copy(f, i).start()

    def forward(f, i):
        ag_copy(f, i).wait_recv()

        @pl.when(far[f] > 0)
        def _():
            ag_copy(f, i).start()

    def step(s, carry):
        for f in range(2):
            i = s - RS_LAG * far[f]

            @pl.when((i >= 0) & (i < items))
            def _():
                compute_part(f, i)

        for f in range(2):
            h = s - RS_LAG * last - AG_LAG * (last - far[f])

            @pl.when((h >= 0) & (h < items) & (far[f] < last))
            def _():
                forward(f, h)

            i = s - RS_LAG * far[f]

            @pl.when((i >= 0) & (i < items))
            def _():
                finish_part(f, i)

        return carry

    lax.fori_loop(0, items + (RS_LAG + AG_LAG) * last, step, 0)

    loads[-1].wait()

    def ret_copy(c, k, target, source):
        return pltpu.make_async_remote_copy(
            src_ref=ret_out_ref.at[c, target], dst_ref=ret_in_ref.at[c, source],
            send_sem=ret_send.at[c, k], recv_sem=ret_recv.at[c, source],
            device_id={"expert": peers[k]}, device_id_type=MESH)

    width = cols // OUT_CHUNKS
    mixed_in = jnp.concatenate([hidden_ref[f, i] for f in range(2) for i in range(items)], axis=1)
    for c in range(OUT_CHUNKS):
        down = wd_ref[:, :, c * width:(c + 1) * width].reshape(held * ff, width)
        own_ref[...] = jnp.dot(mixed_in, down, preferred_element_type=jnp.float32).reshape(n_expert, tok_rows, width)
        ret_out_ref[c] = own_ref[...].astype(jnp.bfloat16)
        for k in range(n_expert - 1):
            ret_copy(c, k, peers[k], me).start()
        ret_in_ref[c, me] = own_ref[me].astype(jnp.bfloat16)
    for c in range(OUT_CHUNKS):
        for k in range(n_expert - 1):
            ret_copy(c, k, peers[k], peers[k]).wait_recv()
        total = jnp.sum(ret_in_ref[c].astype(jnp.float32), axis=0)
        out_ref[:, c * width:(c + 1) * width] = total.astype(jnp.bfloat16)

    for k in range(n_expert - 1):
        tok_copy(k, me).wait_send()
        route_copy(k, me).wait_send()
        for c in range(OUT_CHUNKS):
            ret_copy(c, k, peers[k], me).wait_send()

    def drain(i, carry):
        for f in range(2):
            @pl.when(far[f] < last)
            def _():
                rs_copy(f, i).wait_send()

            @pl.when(far[f] > 0)
            def _():
                ag_copy(f, i).wait_send()

        return carry

    lax.fori_loop(0, items, drain, 0)


def every_expert(tokens, w_gate, w_up, w_down, expert_ids, route_weights):
    n_expert = lax.axis_size("expert")
    n_tensor = lax.axis_size("tensor")
    held, depth, ff = w_gate.shape
    tok_rows, cols = tokens.shape
    all_rows = n_expert * tok_rows
    items = held * (ff // LANES) // 2
    width = cols // OUT_CHUNKS
    labels = jnp.arange(LANES, dtype=jnp.int32)
    chosen = expert_ids[:, :, None] == labels[None, None, :]
    routes = jnp.sum(jnp.where(chosen, route_weights[:, :, None], 0.0), axis=1)
    dma = pltpu.SemaphoreType.DMA
    vmem = pl.BlockSpec(memory_space=pltpu.VMEM)
    hbm = pl.BlockSpec(memory_space=pl.ANY)
    bf16 = jnp.bfloat16
    return pl.pallas_call(
        functools.partial(layer_kernel, n_expert, n_tensor),
        out_shape=jax.ShapeDtypeStruct((tok_rows, cols), bf16),
        in_specs=[vmem, vmem, hbm, hbm, hbm],
        out_specs=vmem,
        scratch_shapes=[
            pltpu.VMEM((n_expert, tok_rows, cols), bf16),
            pltpu.VMEM((n_expert, tok_rows, LANES), jnp.float32),
            pltpu.VMEM((held, all_rows, LANES), jnp.float32),
            pltpu.VMEM(w_gate.shape, bf16),
            pltpu.VMEM(w_up.shape, bf16),
            pltpu.VMEM(w_down.shape, bf16),
            pltpu.VMEM((2, all_rows, 2 * LANES), jnp.float32),
            pltpu.VMEM((2, items, all_rows, 2 * LANES), bf16),
            pltpu.VMEM((2, items, all_rows, 2 * LANES), bf16),
            pltpu.VMEM((2, items, all_rows, LANES), bf16),
            pltpu.VMEM((n_expert, tok_rows, width), jnp.float32),
            pltpu.VMEM((OUT_CHUNKS, n_expert, tok_rows, width), bf16),
            pltpu.VMEM((OUT_CHUNKS, n_expert, tok_rows, width), bf16),
            dma((2 * held + 1,)),
            dma((n_expert - 1,)),
            dma((n_expert,)),
            dma((n_expert - 1,)),
            dma((n_expert,)),
            dma((2, items)),
            dma((2, items)),
            dma((2, items)),
            dma((2, items)),
            dma((OUT_CHUNKS, n_expert - 1)),
            dma((OUT_CHUNKS, n_expert)),
        ],
        compiler_params=pltpu.CompilerParams(
            collective_id=0, has_side_effects=True, vmem_limit_bytes=56 * 1024 * 1024
        ),
    )(tokens, routes, w_gate, w_up, w_down)


def per_device(tokens, w_gate, w_up, w_down, expert_ids, route_weights):
    experts_all = w_gate.shape[0] * lax.axis_size("expert")
    if expert_ids.shape[1] == experts_all:
        return every_expert(tokens, w_gate, w_up, w_down, expert_ids, route_weights)
    return routed_by_slots(tokens, w_gate, w_up, w_down, expert_ids, route_weights)


def solution(mesh):
    in_specs = (
        P(("group", "expert"), "tensor"),
        P("expert", "tensor", None),
        P("expert", "tensor", None),
        P("expert", None, "tensor"),
        P(("group", "expert"), None),
        P(("group", "expert"), None),
    )
    out_specs = P(("group", "expert"), "tensor")
    return jax.shard_map(
        per_device, mesh=mesh, in_specs=in_specs, out_specs=out_specs, check_vma=False
    )
```

```python
import functools

import jax
import jax.numpy as jnp
from jax import lax
from jax.experimental import pallas as pl
from jax.experimental.pallas import tpu as pltpu
from jax.sharding import PartitionSpec as P


def slot_numbers(flat_ids, experts_all):
    labels = jnp.arange(experts_all, dtype=jnp.int32)
    onehot = (flat_ids[:, None] == labels[None, :]).astype(jnp.int32)
    before = jnp.cumsum(onehot, axis=0) - onehot
    return jnp.sum(before * onehot, axis=1)


def routed_by_slots(tokens, w_gate, w_up, w_down, expert_ids, route_weights):
    n_expert = lax.axis_size("expert")
    held_experts = w_gate.shape[0]
    experts_all = held_experts * n_expert
    tok_rows = tokens.shape[0]
    col_share = tokens.shape[1]
    per_token = expert_ids.shape[1]
    capacity = min(tok_rows, 2 * tok_rows * per_token // experts_all)
    flat_ids = expert_ids.reshape(tok_rows * per_token)
    position = flat_ids * capacity + slot_numbers(flat_ids, experts_all)
    owners = jnp.arange(tok_rows * per_token, dtype=jnp.int32) // per_token
    source = jnp.full((experts_all * capacity,), -1, jnp.int32).at[position].set(owners)
    filled = (source >= 0)[:, None]
    picked_rows = jnp.where(filled, tokens[jnp.maximum(source, 0)], jnp.zeros((), tokens.dtype))
    outgoing = picked_rows.reshape(n_expert, held_experts, capacity, col_share)
    received = lax.all_to_all(outgoing, "expert", split_axis=0, concat_axis=0, tiled=True)
    gate_part = jnp.einsum("sjnd,jdf->sjnf", received, w_gate, preferred_element_type=jnp.float32)
    up_part = jnp.einsum("sjnd,jdf->sjnf", received, w_up, preferred_element_type=jnp.float32)
    gate_share = lax.psum_scatter(gate_part, "tensor", scatter_dimension=3, tiled=True)
    up_share = lax.psum_scatter(up_part, "tensor", scatter_dimension=3, tiled=True)
    hidden_share = (jax.nn.silu(gate_share) * up_share).astype(jnp.bfloat16)
    hidden = lax.all_gather(hidden_share, "tensor", axis=3, tiled=True)
    result = jnp.einsum("sjnf,jfd->sjnd", hidden, w_down, preferred_element_type=jnp.float32)
    returned = result.astype(jnp.bfloat16)
    combined = lax.all_to_all(returned, "expert", split_axis=0, concat_axis=0, tiled=True).reshape(
        experts_all * capacity, col_share
    )
    picked = combined[position].reshape(tok_rows, per_token, col_share).astype(jnp.float32)
    mixed_out = jnp.sum(picked * route_weights[:, :, None], axis=1)
    return mixed_out.astype(jnp.bfloat16)


LANES = 128
RS_LAG = 3
AG_LAG = 3
OUT_WIDTH = 256
MESH = pl.DeviceIdType.MESH


def layer_kernel(
    n_expert, n_tensor, tok_ref, ids_ref, weights_ref, wg_hbm, wu_hbm, wd_hbm, out_ref,
    rows_ref, route_ref, routes_ref, scale_ref, wg_ref, wu_ref, wd_ref, part_ref, sent_ref, got_ref, hidden_ref,
    acc_ref, pair_ref, far_out_ref, far_in_ref,
    w_sem, tok_send, tok_recv, pass_send, route_send, route_recv, rs_send, rs_recv, ag_send, ag_recv,
    pair_send, pair_recv, home_send, home_recv,
):
    held, depth, ff = wg_ref.shape
    tok_rows, cols = tok_ref.shape
    all_rows = n_expert * tok_rows
    per_expert = ff // LANES
    items = held * per_expert // 2
    me = lax.axis_index("expert")
    at = lax.axis_index("tensor")
    last = n_tensor - 1
    peers = [lax.rem(me + k, n_expert) for k in range(1, n_expert)]
    chips = n_expert // 2
    core = lax.rem(me, 2)
    chip = me // 2
    partner = 2 * chip + 1 - core
    same = [2 * lax.rem(chip + k, chips) + core for k in range(chips)]
    other = [2 * lax.rem(chip + k, chips) + 1 - core for k in range(chips)]

    loads = []
    for j in range(held):
        for k, (hbm, vmem) in enumerate(((wg_hbm, wg_ref), (wu_hbm, wu_ref))):
            loads.append(pltpu.make_async_copy(hbm.at[j], vmem.at[j], w_sem.at[2 * j + k]))
    loads.append(pltpu.make_async_copy(wd_hbm, wd_ref, w_sem.at[2 * held]))
    for load in loads:
        load.start()

    barrier = pltpu.get_barrier_semaphore()
    for peer in peers:
        pl.semaphore_signal(barrier, inc=1, device_id={"expert": peer}, device_id_type=MESH)

    @pl.when(at > 0)
    def _():
        pl.semaphore_signal(barrier, inc=1, device_id={"tensor": at - 1}, device_id_type=MESH)

    @pl.when(at < last)
    def _():
        pl.semaphore_signal(barrier, inc=1, device_id={"tensor": at + 1}, device_id_type=MESH)

    greeted = (n_expert - 1) + (at > 0).astype(jnp.int32) + (at < last).astype(jnp.int32)
    pl.semaphore_wait(barrier, greeted)

    def tok_copy(k, slot):
        return pltpu.make_async_remote_copy(
            src_ref=tok_ref, dst_ref=rows_ref.at[slot], send_sem=tok_send.at[k], recv_sem=tok_recv.at[slot],
            device_id={"expert": same[k] if k else partner}, device_id_type=MESH)

    def pass_copy(k, slot):
        return pltpu.make_async_remote_copy(
            src_ref=rows_ref.at[slot], dst_ref=rows_ref.at[slot], send_sem=pass_send.at[k],
            recv_sem=tok_recv.at[slot], device_id={"expert": partner}, device_id_type=MESH)

    def route_copy(k, slot):
        return pltpu.make_async_remote_copy(
            src_ref=route_ref, dst_ref=routes_ref.at[slot], send_sem=route_send.at[k], recv_sem=route_recv.at[slot],
            device_id={"expert": peers[k]}, device_id_type=MESH)

    for k in range(chips - 1, -1, -1):
        tok_copy(k, me).start()
    rows_ref[me] = tok_ref[...]
    labels = lax.broadcasted_iota(jnp.int32, (tok_rows, LANES), 1)
    routes = jnp.zeros((tok_rows, LANES), jnp.float32)
    for k in range(ids_ref.shape[1]):
        routes += jnp.where(ids_ref[:, k:k + 1] == labels, weights_ref[:, k:k + 1], 0.0)
    route_ref[...] = routes
    routes_ref[me] = routes
    for k in range(1, chips):
        tok_copy(k, same[k]).wait_recv()
        pass_copy(k, same[k]).start()
    for k in range(n_expert - 1):
        route_copy(k, me).start()
    for load in loads[:-1]:
        load.wait()
    tok_copy(0, partner).wait_recv()
    for k in range(1, chips):
        pass_copy(k, other[k]).wait_recv()

    far = (last - at, at)
    onward = (jnp.maximum(at - 1, 0), jnp.minimum(at + 1, last))
    back = (jnp.minimum(at + 1, last), jnp.maximum(at - 1, 0))

    def rs_copy(f, i):
        return pltpu.make_async_remote_copy(
            src_ref=sent_ref.at[f, i], dst_ref=got_ref.at[f, i], send_sem=rs_send.at[f, i], recv_sem=rs_recv.at[f, i],
            device_id={"tensor": onward[f]}, device_id_type=MESH)

    def ag_copy(f, i):
        return pltpu.make_async_remote_copy(
            src_ref=hidden_ref.at[f, i], dst_ref=hidden_ref.at[f, i], send_sem=ag_send.at[f, i],
            recv_sem=ag_recv.at[f, i], device_id={"tensor": back[f]}, device_id_type=MESH)

    def compute_part(f, i):
        q = f * items + i
        j = q // per_expert
        start = pl.multiple_of(lax.rem(q, per_expert) * LANES, LANES)
        both = jnp.concatenate([wg_ref[j, :, pl.ds(start, LANES)], wu_ref[j, :, pl.ds(start, LANES)]], axis=1)
        part_ref[f] = jnp.dot(rows_ref[...].reshape(all_rows, depth), both, preferred_element_type=jnp.float32)

    def finish_part(f, i):
        @pl.when(far[f] > 0)
        def _():
            rs_copy(f, i).wait_recv()
            part_ref[f] = part_ref[f] + got_ref[f, i].astype(jnp.float32)

        @pl.when(far[f] < last)
        def _():
            sent_ref[f, i] = part_ref[f].astype(jnp.bfloat16)
            rs_copy(f, i).start()

        @pl.when(far[f] == last)
        def _():
            gate = part_ref[f, :, :LANES]
            up = part_ref[f, :, LANES:]
            j = (f * items + i) // per_expert
            hidden_ref[f, i] = (jax.nn.silu(gate) * up * scale_ref[j]).astype(jnp.bfloat16)
            ag_copy(f, i).start()

    def step(s, carry):
        for f in range(2):
            i = s - RS_LAG * far[f]

            @pl.when((i >= 0) & (i < items))
            def _():
                compute_part(f, i)

        for f in range(2):
            i = s - RS_LAG * far[f]

            @pl.when((i >= 0) & (i < items))
            def _():
                finish_part(f, i)

        return carry

    lax.fori_loop(0, RS_LAG * last, step, 0)

    for k in range(n_expert - 1):
        route_copy(k, peers[k]).wait_recv()
    all_routes = routes_ref[...].reshape(all_rows, LANES)
    lane = lax.broadcasted_iota(jnp.int32, (all_rows, LANES), 1)
    for j in range(held):
        mine = jnp.sum(jnp.where(lane == me * held + j, all_routes, 0.0), axis=1, keepdims=True)
        scale_ref[j] = jnp.broadcast_to(mine, (all_rows, LANES))

    lax.fori_loop(RS_LAG * last, items + RS_LAG * last, step, 0)

    loads[-1].wait()
    acc_ref[...] = jnp.zeros_like(acc_ref)

    def collect(s, carry):
        for f in range(2):
            i = s - AG_LAG * (last - far[f])

            @pl.when((i >= 0) & (i < items) & (far[f] < last))
            def _():
                ag_copy(f, i).wait_recv()

                @pl.when(far[f] > 0)
                def _():
                    ag_copy(f, i).start()

        for f in range(2):
            i = s - AG_LAG * (last - far[f])

            @pl.when((i >= 0) & (i < items) & (lax.rem(i + items, 2) == 1))
            def _():
                q = f * items + i - 1
                j = q // per_expert
                start = pl.multiple_of(lax.rem(q, per_expert) * LANES, LANES)
                pair = jnp.concatenate([hidden_ref[f, i - 1], hidden_ref[f, i]], axis=1)
                for c in range(0, cols, OUT_WIDTH):
                    down = wd_ref[j, pl.ds(start, 2 * LANES), c:c + OUT_WIDTH]
                    term = jnp.dot(pair, down, preferred_element_type=jnp.float32)
                    acc_ref[:, :, c:c + OUT_WIDTH] += term.reshape(n_expert, tok_rows, OUT_WIDTH)

        return carry

    lax.fori_loop(0, items + AG_LAG * last, collect, 0)

    def pair_copy(k):
        return pltpu.make_async_remote_copy(
            src_ref=acc_ref.at[other[k]], dst_ref=pair_ref.at[k], send_sem=pair_send.at[k],
            recv_sem=pair_recv.at[k], device_id={"expert": partner}, device_id_type=MESH)

    def home_copy(k):
        return pltpu.make_async_remote_copy(
            src_ref=far_out_ref.at[k], dst_ref=far_in_ref.at[k], send_sem=home_send.at[k],
            recv_sem=home_recv.at[k], device_id={"expert": same[k]}, device_id_type=MESH)

    for k in range(chips - 1, -1, -1):
        pair_copy(k).start()
    for k in range(1, chips):
        pair_copy(k).wait_recv()
        far_out_ref[k] = (acc_ref[same[k]] + pair_ref[k]).astype(jnp.bfloat16)
        home_copy(k).start()

    for k in range(chips):
        tok_copy(k, me).wait_send()
        pair_copy(k).wait_send()
        if k:
            pass_copy(k, same[k]).wait_send()
    for k in range(n_expert - 1):
        route_copy(k, me).wait_send()

    def drain(i, carry):
        for f in range(2):
            @pl.when(far[f] < last)
            def _():
                rs_copy(f, i).wait_send()

            @pl.when(far[f] > 0)
            def _():
                ag_copy(f, i).wait_send()

        return carry

    lax.fori_loop(0, items, drain, 0)

    pair_copy(0).wait_recv()
    acc_ref[me] += pair_ref[0]
    total = acc_ref[me]
    for k in range(1, chips):
        home_copy(k).wait_recv()
        total = total + far_in_ref[k].astype(jnp.float32)
    out_ref[...] = total.astype(jnp.bfloat16)
    for k in range(1, chips):
        home_copy(k).wait_send()


def every_expert(tokens, w_gate, w_up, w_down, expert_ids, route_weights):
    n_expert = lax.axis_size("expert")
    n_tensor = lax.axis_size("tensor")
    held, depth, ff = w_gate.shape
    tok_rows, cols = tokens.shape
    all_rows = n_expert * tok_rows
    items = held * (ff // LANES) // 2
    chips = n_expert // 2
    dma = pltpu.SemaphoreType.DMA
    vmem = pl.BlockSpec(memory_space=pltpu.VMEM)
    hbm = pl.BlockSpec(memory_space=pl.ANY)
    bf16 = jnp.bfloat16
    return pl.pallas_call(
        functools.partial(layer_kernel, n_expert, n_tensor),
        out_shape=jax.ShapeDtypeStruct((tok_rows, cols), bf16),
        in_specs=[vmem, vmem, vmem, hbm, hbm, hbm],
        out_specs=vmem,
        scratch_shapes=[
            pltpu.VMEM((n_expert, tok_rows, cols), bf16),
            pltpu.VMEM((tok_rows, LANES), jnp.float32),
            pltpu.VMEM((n_expert, tok_rows, LANES), jnp.float32),
            pltpu.VMEM((held, all_rows, LANES), jnp.float32),
            pltpu.VMEM(w_gate.shape, bf16),
            pltpu.VMEM(w_up.shape, bf16),
            pltpu.VMEM(w_down.shape, bf16),
            pltpu.VMEM((2, all_rows, 2 * LANES), jnp.float32),
            pltpu.VMEM((2, items, all_rows, 2 * LANES), bf16),
            pltpu.VMEM((2, items, all_rows, 2 * LANES), bf16),
            pltpu.VMEM((2, items, all_rows, LANES), bf16),
            pltpu.VMEM((n_expert, tok_rows, cols), jnp.float32),
            pltpu.VMEM((chips, tok_rows, cols), jnp.float32),
            pltpu.VMEM((chips, tok_rows, cols), bf16),
            pltpu.VMEM((chips, tok_rows, cols), bf16),
            dma((2 * held + 1,)),
            dma((chips,)),
            dma((n_expert,)),
            dma((chips,)),
            dma((n_expert - 1,)),
            dma((n_expert,)),
            dma((2, items)),
            dma((2, items)),
            dma((2, items)),
            dma((2, items)),
            dma((chips,)),
            dma((chips,)),
            dma((chips,)),
            dma((chips,)),
        ],
        compiler_params=pltpu.CompilerParams(
            collective_id=0, has_side_effects=True, vmem_limit_bytes=56 * 1024 * 1024
        ),
    )(tokens, expert_ids, route_weights, w_gate, w_up, w_down)


def per_device(tokens, w_gate, w_up, w_down, expert_ids, route_weights):
    experts_all = w_gate.shape[0] * lax.axis_size("expert")
    if expert_ids.shape[1] == experts_all:
        return every_expert(tokens, w_gate, w_up, w_down, expert_ids, route_weights)
    return routed_by_slots(tokens, w_gate, w_up, w_down, expert_ids, route_weights)


def solution(mesh):
    in_specs = (
        P(("group", "expert"), "tensor"),
        P("expert", "tensor", None),
        P("expert", "tensor", None),
        P("expert", None, "tensor"),
        P(("group", "expert"), None),
        P(("group", "expert"), None),
    )
    out_specs = P(("group", "expert"), "tensor")
    return jax.shard_map(
        per_device, mesh=mesh, in_specs=in_specs, out_specs=out_specs, check_vma=False
    )
```

```python
import functools

import jax
import jax.numpy as jnp
from jax import lax
from jax.experimental import pallas as pl
from jax.experimental.pallas import tpu as pltpu
from jax.sharding import PartitionSpec as P


def slot_numbers(flat_ids, experts_all):
    labels = jnp.arange(experts_all, dtype=jnp.int32)
    onehot = (flat_ids[:, None] == labels[None, :]).astype(jnp.int32)
    before = jnp.cumsum(onehot, axis=0) - onehot
    return jnp.sum(before * onehot, axis=1)


def routed_by_slots(tokens, w_gate, w_up, w_down, expert_ids, route_weights):
    n_expert = lax.axis_size("expert")
    held_experts = w_gate.shape[0]
    experts_all = held_experts * n_expert
    tok_rows = tokens.shape[0]
    col_share = tokens.shape[1]
    per_token = expert_ids.shape[1]
    capacity = min(tok_rows, 2 * tok_rows * per_token // experts_all)
    flat_ids = expert_ids.reshape(tok_rows * per_token)
    position = flat_ids * capacity + slot_numbers(flat_ids, experts_all)
    owners = jnp.arange(tok_rows * per_token, dtype=jnp.int32) // per_token
    source = jnp.full((experts_all * capacity,), -1, jnp.int32).at[position].set(owners)
    filled = (source >= 0)[:, None]
    picked_rows = jnp.where(filled, tokens[jnp.maximum(source, 0)], jnp.zeros((), tokens.dtype))
    outgoing = picked_rows.reshape(n_expert, held_experts, capacity, col_share)
    received = lax.all_to_all(outgoing, "expert", split_axis=0, concat_axis=0, tiled=True)
    gate_part = jnp.einsum("sjnd,jdf->sjnf", received, w_gate, preferred_element_type=jnp.float32)
    up_part = jnp.einsum("sjnd,jdf->sjnf", received, w_up, preferred_element_type=jnp.float32)
    gate_share = lax.psum_scatter(gate_part, "tensor", scatter_dimension=3, tiled=True)
    up_share = lax.psum_scatter(up_part, "tensor", scatter_dimension=3, tiled=True)
    hidden_share = (jax.nn.silu(gate_share) * up_share).astype(jnp.bfloat16)
    hidden = lax.all_gather(hidden_share, "tensor", axis=3, tiled=True)
    result = jnp.einsum("sjnf,jfd->sjnd", hidden, w_down, preferred_element_type=jnp.float32)
    returned = result.astype(jnp.bfloat16)
    combined = lax.all_to_all(returned, "expert", split_axis=0, concat_axis=0, tiled=True).reshape(
        experts_all * capacity, col_share
    )
    picked = combined[position].reshape(tok_rows, per_token, col_share).astype(jnp.float32)
    mixed_out = jnp.sum(picked * route_weights[:, :, None], axis=1)
    return mixed_out.astype(jnp.bfloat16)


LANES = 128
RS_LAG = 3
AG_LAG = 3
OUT_WIDTH = 256
MESH = pl.DeviceIdType.MESH


def layer_kernel(
    n_expert, n_tensor, tok_ref, ids_ref, weights_ref, wg_hbm, wu_hbm, wd_hbm, out_ref,
    rows_ref, route_ref, routes_ref, scale_ref, wg_ref, wu_ref, wd_ref, part_ref, sent_ref, got_ref, hidden_ref,
    acc_ref, pair_ref, far_out_ref, far_in_ref,
    w_sem, tok_send, tok_recv, pass_send, route_send, route_recv, rs_send, rs_recv, ag_send, ag_recv,
    pair_send, pair_recv, home_send, home_recv,
):
    held, depth, ff = wg_ref.shape
    tok_rows, cols = tok_ref.shape
    all_rows = n_expert * tok_rows
    per_expert = ff // LANES
    items = held * per_expert // 2
    me = lax.axis_index("expert")
    at = lax.axis_index("tensor")
    last = n_tensor - 1
    peers = [lax.rem(me + k, n_expert) for k in range(1, n_expert)]
    chips = n_expert // 2
    core = lax.rem(me, 2)
    chip = me // 2
    partner = 2 * chip + 1 - core
    same = [2 * lax.rem(chip + k, chips) + core for k in range(chips)]
    other = [2 * lax.rem(chip + k, chips) + 1 - core for k in range(chips)]

    loads = []
    for j in range(held):
        for k, (hbm, vmem) in enumerate(((wg_hbm, wg_ref), (wu_hbm, wu_ref))):
            loads.append(pltpu.make_async_copy(hbm.at[j], vmem.at[j], w_sem.at[2 * j + k]))
    loads.append(pltpu.make_async_copy(wd_hbm, wd_ref, w_sem.at[2 * held]))
    for load in loads:
        load.start()

    barrier = pltpu.get_barrier_semaphore()
    for peer in peers:
        pl.semaphore_signal(barrier, inc=1, device_id={"expert": peer}, device_id_type=MESH)

    @pl.when(at > 0)
    def _():
        pl.semaphore_signal(barrier, inc=1, device_id={"tensor": at - 1}, device_id_type=MESH)

    @pl.when(at < last)
    def _():
        pl.semaphore_signal(barrier, inc=1, device_id={"tensor": at + 1}, device_id_type=MESH)

    greeted = (n_expert - 1) + (at > 0).astype(jnp.int32) + (at < last).astype(jnp.int32)
    pl.semaphore_wait(barrier, greeted)

    def tok_copy(k, slot):
        return pltpu.make_async_remote_copy(
            src_ref=tok_ref, dst_ref=rows_ref.at[slot], send_sem=tok_send.at[k], recv_sem=tok_recv.at[slot],
            device_id={"expert": same[k] if k else partner}, device_id_type=MESH)

    def pass_copy(k, slot):
        return pltpu.make_async_remote_copy(
            src_ref=rows_ref.at[slot], dst_ref=rows_ref.at[slot], send_sem=pass_send.at[k],
            recv_sem=tok_recv.at[slot], device_id={"expert": partner}, device_id_type=MESH)

    def route_copy(k, slot):
        return pltpu.make_async_remote_copy(
            src_ref=route_ref, dst_ref=routes_ref.at[slot], send_sem=route_send.at[k], recv_sem=route_recv.at[slot],
            device_id={"expert": peers[k]}, device_id_type=MESH)

    for k in range(chips - 1, -1, -1):
        tok_copy(k, me).start()
    rows_ref[me] = tok_ref[...]
    for k in range(1, chips):
        tok_copy(k, same[k]).wait_recv()
        pass_copy(k, same[k]).start()
    labels = lax.broadcasted_iota(jnp.int32, (tok_rows, LANES), 1)
    routes = jnp.zeros((tok_rows, LANES), jnp.float32)
    for k in range(ids_ref.shape[1]):
        routes += jnp.where(ids_ref[:, k:k + 1] == labels, weights_ref[:, k:k + 1], 0.0)
    route_ref[...] = routes
    routes_ref[me] = routes
    for k in range(n_expert - 1):
        route_copy(k, me).start()
    for load in loads[:-1]:
        load.wait()
    tok_copy(0, partner).wait_recv()
    for k in range(1, chips):
        pass_copy(k, other[k]).wait_recv()

    far = (last - at, at)
    onward = (jnp.maximum(at - 1, 0), jnp.minimum(at + 1, last))
    back = (jnp.minimum(at + 1, last), jnp.maximum(at - 1, 0))

    def rs_copy(f, i):
        return pltpu.make_async_remote_copy(
            src_ref=sent_ref.at[f, i], dst_ref=got_ref.at[f, i], send_sem=rs_send.at[f, i], recv_sem=rs_recv.at[f, i],
            device_id={"tensor": onward[f]}, device_id_type=MESH)

    def ag_copy(f, i):
        return pltpu.make_async_remote_copy(
            src_ref=hidden_ref.at[f, i], dst_ref=hidden_ref.at[f, i], send_sem=ag_send.at[f, i],
            recv_sem=ag_recv.at[f, i], device_id={"tensor": back[f]}, device_id_type=MESH)

    def compute_part(f, i):
        q = f * items + i
        j = q // per_expert
        start = pl.multiple_of(lax.rem(q, per_expert) * LANES, LANES)
        both = jnp.concatenate([wg_ref[j, :, pl.ds(start, LANES)], wu_ref[j, :, pl.ds(start, LANES)]], axis=1)
        part_ref[f] = jnp.dot(rows_ref[...].reshape(all_rows, depth), both, preferred_element_type=jnp.float32)

    def finish_part(f, i):
        @pl.when(far[f] > 0)
        def _():
            rs_copy(f, i).wait_recv()
            part_ref[f] = part_ref[f] + got_ref[f, i].astype(jnp.float32)

        @pl.when(far[f] < last)
        def _():
            sent_ref[f, i] = part_ref[f].astype(jnp.bfloat16)
            rs_copy(f, i).start()

        @pl.when(far[f] == last)
        def _():
            gate = part_ref[f, :, :LANES]
            up = part_ref[f, :, LANES:]
            j = (f * items + i) // per_expert
            hidden_ref[f, i] = (jax.nn.silu(gate) * up * scale_ref[j]).astype(jnp.bfloat16)
            ag_copy(f, i).start()

    def step(s, carry):
        for f in range(2):
            i = s - RS_LAG * far[f]

            @pl.when((i >= 0) & (i < items))
            def _():
                compute_part(f, i)

        for f in range(2):
            i = s - RS_LAG * far[f]

            @pl.when((i >= 0) & (i < items))
            def _():
                finish_part(f, i)

        return carry

    lax.fori_loop(0, RS_LAG * last, step, 0)

    for k in range(n_expert - 1):
        route_copy(k, peers[k]).wait_recv()
    all_routes = routes_ref[...].reshape(all_rows, LANES)
    lane = lax.broadcasted_iota(jnp.int32, (all_rows, LANES), 1)
    for j in range(held):
        mine = jnp.sum(jnp.where(lane == me * held + j, all_routes, 0.0), axis=1, keepdims=True)
        scale_ref[j] = jnp.broadcast_to(mine, (all_rows, LANES))

    lax.fori_loop(RS_LAG * last, items + RS_LAG * last, step, 0)

    loads[-1].wait()
    acc_ref[...] = jnp.zeros_like(acc_ref)

    def collect(s, carry):
        for f in range(2):
            i = s - AG_LAG * (last - far[f])

            @pl.when((i >= 0) & (i < items) & (far[f] < last))
            def _():
                ag_copy(f, i).wait_recv()

                @pl.when(far[f] > 0)
                def _():
                    ag_copy(f, i).start()

        for f in range(2):
            i = s - AG_LAG * (last - far[f])

            @pl.when((i >= 0) & (i < items) & (lax.rem(i + items, 2) == 1))
            def _():
                q = f * items + i - 1
                j = q // per_expert
                start = pl.multiple_of(lax.rem(q, per_expert) * LANES, LANES)
                pair = jnp.concatenate([hidden_ref[f, i - 1], hidden_ref[f, i]], axis=1)
                for c in range(0, cols, OUT_WIDTH):
                    down = wd_ref[j, pl.ds(start, 2 * LANES), c:c + OUT_WIDTH]
                    term = jnp.dot(pair, down, preferred_element_type=jnp.float32)
                    acc_ref[:, :, c:c + OUT_WIDTH] += term.reshape(n_expert, tok_rows, OUT_WIDTH)

        return carry

    lax.fori_loop(0, items + AG_LAG * last, collect, 0)

    def pair_copy(k):
        return pltpu.make_async_remote_copy(
            src_ref=acc_ref.at[other[k]], dst_ref=pair_ref.at[k], send_sem=pair_send.at[k],
            recv_sem=pair_recv.at[k], device_id={"expert": partner}, device_id_type=MESH)

    def home_copy(k):
        return pltpu.make_async_remote_copy(
            src_ref=far_out_ref.at[k], dst_ref=far_in_ref.at[k], send_sem=home_send.at[k],
            recv_sem=home_recv.at[k], device_id={"expert": same[k]}, device_id_type=MESH)

    for k in range(chips - 1, -1, -1):
        pair_copy(k).start()
    for k in range(1, chips):
        pair_copy(k).wait_recv()
        far_out_ref[k] = (acc_ref[same[k]] + pair_ref[k]).astype(jnp.bfloat16)
        home_copy(k).start()

    for k in range(chips):
        tok_copy(k, me).wait_send()
        pair_copy(k).wait_send()
        if k:
            pass_copy(k, same[k]).wait_send()
    for k in range(n_expert - 1):
        route_copy(k, me).wait_send()

    def drain(i, carry):
        for f in range(2):
            @pl.when(far[f] < last)
            def _():
                rs_copy(f, i).wait_send()

            @pl.when(far[f] > 0)
            def _():
                ag_copy(f, i).wait_send()

        return carry

    lax.fori_loop(0, items, drain, 0)

    pair_copy(0).wait_recv()
    acc_ref[me] += pair_ref[0]
    total = acc_ref[me]
    for k in range(1, chips):
        home_copy(k).wait_recv()
        total = total + far_in_ref[k].astype(jnp.float32)
    out_ref[...] = total.astype(jnp.bfloat16)
    for k in range(1, chips):
        home_copy(k).wait_send()


def every_expert(tokens, w_gate, w_up, w_down, expert_ids, route_weights):
    n_expert = lax.axis_size("expert")
    n_tensor = lax.axis_size("tensor")
    held, depth, ff = w_gate.shape
    tok_rows, cols = tokens.shape
    all_rows = n_expert * tok_rows
    items = held * (ff // LANES) // 2
    chips = n_expert // 2
    dma = pltpu.SemaphoreType.DMA
    vmem = pl.BlockSpec(memory_space=pltpu.VMEM)
    hbm = pl.BlockSpec(memory_space=pl.ANY)
    bf16 = jnp.bfloat16
    return pl.pallas_call(
        functools.partial(layer_kernel, n_expert, n_tensor),
        out_shape=jax.ShapeDtypeStruct((tok_rows, cols), bf16),
        in_specs=[vmem, vmem, vmem, hbm, hbm, hbm],
        out_specs=vmem,
        scratch_shapes=[
            pltpu.VMEM((n_expert, tok_rows, cols), bf16),
            pltpu.VMEM((tok_rows, LANES), jnp.float32),
            pltpu.VMEM((n_expert, tok_rows, LANES), jnp.float32),
            pltpu.VMEM((held, all_rows, LANES), jnp.float32),
            pltpu.VMEM(w_gate.shape, bf16),
            pltpu.VMEM(w_up.shape, bf16),
            pltpu.VMEM(w_down.shape, bf16),
            pltpu.VMEM((2, all_rows, 2 * LANES), jnp.float32),
            pltpu.VMEM((2, items, all_rows, 2 * LANES), bf16),
            pltpu.VMEM((2, items, all_rows, 2 * LANES), bf16),
            pltpu.VMEM((2, items, all_rows, LANES), bf16),
            pltpu.VMEM((n_expert, tok_rows, cols), jnp.float32),
            pltpu.VMEM((chips, tok_rows, cols), jnp.float32),
            pltpu.VMEM((chips, tok_rows, cols), bf16),
            pltpu.VMEM((chips, tok_rows, cols), bf16),
            dma((2 * held + 1,)),
            dma((chips,)),
            dma((n_expert,)),
            dma((chips,)),
            dma((n_expert - 1,)),
            dma((n_expert,)),
            dma((2, items)),
            dma((2, items)),
            dma((2, items)),
            dma((2, items)),
            dma((chips,)),
            dma((chips,)),
            dma((chips,)),
            dma((chips,)),
        ],
        compiler_params=pltpu.CompilerParams(
            collective_id=0, has_side_effects=True, vmem_limit_bytes=56 * 1024 * 1024
        ),
    )(tokens, expert_ids, route_weights, w_gate, w_up, w_down)


def per_device(tokens, w_gate, w_up, w_down, expert_ids, route_weights):
    experts_all = w_gate.shape[0] * lax.axis_size("expert")
    if expert_ids.shape[1] == experts_all:
        return every_expert(tokens, w_gate, w_up, w_down, expert_ids, route_weights)
    return routed_by_slots(tokens, w_gate, w_up, w_down, expert_ids, route_weights)


def solution(mesh):
    in_specs = (
        P(("group", "expert"), "tensor"),
        P("expert", "tensor", None),
        P("expert", "tensor", None),
        P("expert", None, "tensor"),
        P(("group", "expert"), None),
        P(("group", "expert"), None),
    )
    out_specs = P(("group", "expert"), "tensor")
    return jax.shard_map(
        per_device, mesh=mesh, in_specs=in_specs, out_specs=out_specs, check_vma=False
    )
```
